32 devices in a mesh: groups: 2 (over y), row: 4 (over z), col: 4 (over x, core).
Axes of the slice: x: 2, y: 2, z: 4, core: 2. Of those that a mesh axis runs over, the one named last changes fastest.
Arguments:
- factors: float32 [8, 1280, 5120], P('groups', 'row', 'col'), parts along dimension 0, may hold values from -1.5 to 1.5, as said below
- right_side: float32 [8, 1280, 96], P(('groups', 'col'), 'row'), parts along dimension 0, may hold values from -6 to 6
Outputs:
- forward: float32 [8, 1280, 96], P(('groups', 'col'), 'row'), parts along dimension 0
- solution: float32 [8, 1280, 96], P(('groups', 'col'), 'row'), parts along dimension 0
The draws below stay inside these ranges and needn't reach their ends.
There are 2 independent parts, one for each index of `groups`. The reference program is written for one: setup_inputs(seed, part) draws one part's arguments, and reference() takes and returns one part's arrays. A program takes and returns all parts, laid end to end along the dimension named above; each array names one. Nothing has to cross between parts.
Inputs may be any that keep to these rules, and one draw needn't show every extreme that they name: `factors`: off the diagonal tiles, the entries are those of L below and of U above. Diagonal tile k holds, strictly below its diagonal, the strictly lower part of the inverse of L's unit lower triangular diagonal tile, and on and above its diagonal the inverse of U's upper triangular diagonal tile.
All inputs are finite; a program needn't handle non-finite values.
Results may differ from the reference program's by a relative error of at most 0.00014.
Values sent between devices are 32-bit elements; how exact they have to be, the bound alone decides.
A program may use at most 128 MiB of HBM per device.

```python
import math
import jax
import jax.numpy as jnp
from jax import lax

TS = 1280
R = 96
TILES = 4


def draw_factors(key, part):
    first, second = jax.random.split(jax.random.fold_in(key, 11))
    shape = (TILES, TS, TILES * TS)
    base = jnp.clip(jax.random.normal(first, shape, jnp.float32), -4.0, 4.0)
    pivots = jax.random.uniform(second, shape, jnp.float32, 0.5, 1.5)
    tile_ids = jnp.arange(TILES)[:, None, None]
    inner = jnp.arange(TS)[None, :, None]
    columns = jnp.arange(TILES * TS)[None, None, :]
    same = columns // TS == tile_ids
    local = columns % TS
    scaled = jnp.where(same, base * (0.5 / math.sqrt(TS)), base * (1.0 / math.sqrt(TILES * TS)))
    return jnp.where(same & (local == inner), pivots, scaled)


def level_of(rng, dims, cuts, low, top_value):
    loudness, own = 1.0, jax.random.fold_in(rng, 6)
    for dim, parts in cuts:
        steps = jnp.exp(jax.random.uniform(jax.random.fold_in(own, dim), (parts,), jnp.float32, low / len(cuts), top_value / len(cuts)))
        loudness = loudness * jnp.repeat(steps, dims[dim] // parts).reshape([-1 if axis == dim else 1 for axis in range(len(dims))])
    return loudness


def gaussian(rng, shape, spread, reach, pieces=(), kind=jnp.bfloat16):
    result = jax.random.normal(rng, shape, jnp.float32) * spread
    if len(pieces) > 0:
        result = level_of(rng, shape, pieces, -0.22, 0.18) * result
    return jnp.clip(result, min=-reach, max=reach).astype(kind)


def setup_inputs(seed: int = 0, part: int = 0) -> dict:
    splits = jax.random.split(jax.random.key(seed), 3)
    part_keys = jax.random.split(jax.random.fold_in(splits[2], part), 3)
    return {
        "factors": draw_factors(jax.random.fold_in(jax.random.fold_in(splits[2], part), 71), part),
        "right_side": gaussian(part_keys[1], (TILES, TS, R), 1.0, 6.0, ((0, 4), (1, 4)), jnp.float32),
    }


def reference(factors, right_side):
    row_ids = jnp.arange(TS)[:, None]
    col_ids = jnp.arange(TS)[None, :]
    forward = []
    for current in range(TILES):
        vector = right_side[current]
        if current > 0:
            earlier = jnp.concatenate(forward, 0)
            vector = vector - jnp.dot(factors[current, :, :current * TS], earlier, preferred_element_type=jnp.float32, precision=lax.Precision.HIGHEST)
        diagonal = factors[current, :, current * TS:(current + 1) * TS]
        lower = jnp.where(col_ids < row_ids, diagonal, 0.0) + (col_ids == row_ids).astype(diagonal.dtype)
        forward.append(jnp.dot(lower, vector, preferred_element_type=jnp.float32, precision=lax.Precision.HIGHEST))
    solution = [None] * TILES
    for current in range(TILES - 1, -1, -1):
        vector = forward[current]
        if current < TILES - 1:
            later = jnp.concatenate(solution[current + 1:], 0)
            vector = vector - jnp.dot(factors[current, :, (current + 1) * TS:], later, preferred_element_type=jnp.float32, precision=lax.Precision.HIGHEST)
        diagonal = factors[current, :, current * TS:(current + 1) * TS]
        upper = jnp.where(col_ids >= row_ids, diagonal, 0.0)
        solution[current] = jnp.dot(upper, vector, preferred_element_type=jnp.float32, precision=lax.Precision.HIGHEST)
    return jnp.stack(forward), jnp.stack(solution)
```

```python
import functools

import jax
import jax.numpy as jnp
from jax import lax
from jax.experimental import pallas as pl
from jax.experimental.pallas import tpu as pltpu
from jax.sharding import PartitionSpec as P

MESH = pl.DeviceIdType.MESH
CHUNKS = 6
TURN = 256


def kernel(
    n_row, n_col, chunks, rows, size, width,
    factors_hbm, rs_ref,
    fwd_ref, sol_ref,
    raw, turned, corner, ahi, alo, v_buf, f_buf, w_buf, s_buf, t_buf, tb_buf, rin, rout, rbin, rbout,
    a_sem, v_send, v_recv, f_send, f_recv, w_send, w_recv, s_send, s_recv,
    r_send, r_recv, rb_send, rb_recv, b0_send,
):
    r = lax.axis_index("row")
    c = lax.axis_index("col")
    last = n_col - 1
    portion = width // chunks
    short = n_row <= 4

    def load(k):
        return pltpu.make_async_copy(factors_hbm.at[k], raw.at[k, pl.ds(0, rows), :], a_sem.at[k])

    def start_load(i, _):
        load(lax.rem(c + i, n_col)).start()
        return 0

    lax.fori_loop(0, n_col, start_load, 0)

    barrier = pltpu.get_barrier_semaphore()

    def greet(i, _):
        rr, cc = i // n_col, i % n_col

        @pl.when(i != r * n_col + c)
        def _():
            pl.semaphore_signal(barrier, inc=1, device_id={"row": rr, "col": cc}, device_id_type=MESH)

        return 0

    lax.fori_loop(0, n_row * n_col, greet, 0)
    pl.semaphore_wait(barrier, n_row * n_col - 1)

    def remote(src, dst, send, recv, row, col):
        return pltpu.make_async_remote_copy(
            src_ref=src, dst_ref=dst, send_sem=send, recv_sem=recv,
            device_id={"row": row, "col": col}, device_id_type=MESH,
        )

    def each_chunk(body):
        def step(q, _):
            body(q)
            return 0

        lax.fori_loop(0, chunks, step, 0)

    def each_row(body):
        def step(s, _):
            body(s)
            return 0

        lax.fori_loop(0, n_row, step, 0, unroll=short)

    def far_first(body, up, down, own):
        def step(i, _):
            d = n_row - 1 - i
            if up:
                @pl.when(r + d < n_row)
                def _():
                    body(r + d)

            if down:
                @pl.when(r - d >= 0)
                def _():
                    body(r - d)

            return 0

        lax.fori_loop(0, n_row - 1, step, 0, unroll=short)
        if own:
            body(r)

    def split(x):
        hi = x.astype(jnp.bfloat16)
        return hi, (x - hi.astype(jnp.float32)).astype(jnp.bfloat16)

    def combine(buf, k, q):
        def step(s, acc):
            hi, lo = split(buf[q, s])
            both = jnp.concatenate([hi, lo], axis=0)
            one = jnp.dot(both, ahi[k, s], preferred_element_type=jnp.float32)
            two = jnp.dot(hi, alo[k, s], preferred_element_type=jnp.float32)
            return acc + (one[:portion] + one[portion:] + two)

        zero = jnp.zeros((portion, rows), jnp.float32)
        return lax.fori_loop(0, n_row, step, zero, unroll=short)

    def arrive(buf, recv, q, s):
        remote(buf.at[q, s], buf.at[q, s], recv.at[q, s], recv.at[q, s], r, c).wait_recv()

    def arrivals(buf, recv, q, up, down, own):
        def one(s):
            wanted = None if own else s != r
            if not up:
                wanted = s <= r if own else s < r
            if not down:
                wanted = s >= r if own else s > r
            if wanted is None:
                arrive(buf, recv, q, s)
            else:
                @pl.when(wanted)
                def _():
                    arrive(buf, recv, q, s)

        each_row(one)

    def chunk(ref, q):
        return ref.at[0, pl.ds(pl.multiple_of(q * portion, 8), portion), :]

    def to_row(src, buf, send, recv, q, row, col):
        return remote(src, buf.at[q, r], send.at[q, row], recv.at[q, r], row, col)

    @pl.when(c == 0)
    def _():
        def one(q):
            far_first(lambda row: to_row(chunk(rs_ref, q), v_buf, v_send, v_recv, q, row, c).start(), True, False, False)
            v_buf[q, r] = chunk(rs_ref, q)[...]

        each_chunk(one)

    def first_run(q):
        return remote(chunk(rs_ref, q), rin.at[c, q], r_send.at[c, q], r_recv.at[c, q], r, 0)

    @pl.when(c > 0)
    def _():
        each_chunk(lambda q: first_run(q).start())

    def blank(s):
        zero = jnp.zeros((chunks, portion, rows), jnp.float32)

        @pl.when(s > r)
        def _():
            v_buf[:, s] = zero

        @pl.when(s < r)
        def _():
            w_buf[:, s] = zero

            @pl.when(c == last)
            def _():
                f_buf[:, s] = zero

    each_row(blank)

    def turn(k):
        def step(j, _):
            base = pl.multiple_of(j * TURN, TURN)
            turned[pl.ds(base, TURN), :] = raw[k, :, pl.ds(base, TURN)].T
            return 0

        load(k).wait()
        lax.fori_loop(0, size // TURN, step, 0)

        def cut(s, _):
            hi, lo = split(turned[pl.ds(pl.multiple_of(s * rows, 8), rows), :rows])
            ahi[k, s] = hi
            alo[k, s] = lo
            return 0

        lax.fori_loop(0, n_row, cut, 0)

    def place():
        return lax.broadcasted_iota(jnp.int32, (rows, rows), 0), lax.broadcasted_iota(jnp.int32, (rows, rows), 1)

    def set_lower():
        column, line = place()
        value = turned[pl.ds(pl.multiple_of(r * rows, 8), rows), :rows]
        corner[...] = value
        value = jnp.where(column < line, value, jnp.where(column == line, 1.0, 0.0))
        ahi[c, r], alo[c, r] = split(value)

    def set_upper():
        column, line = place()
        ahi[c, r], alo[c, r] = split(jnp.where(column >= line, corner[...], 0.0))

    turn(c)
    set_lower()

    @pl.when(c == 0)
    def _():
        turn(c + 1)

    @pl.when(c > 0)
    def _():
        def step(i, _):
            turn(lax.rem(c + i, n_col))
            return 0

        lax.fori_loop(1, n_col, step, 0)

    def back_run(q):
        return remote(f_buf.at[q, r], rbin.at[c, q], b0_send.at[q], rb_recv.at[c, q], r, last)

    def deliver(ref, q, value):
        ref[0, pl.ds(pl.multiple_of(q * portion, 8), portion), :] = value

    def solve_forward(own):
        def one(q):
            arrivals(v_buf, v_recv, q, False, True, own)
            acc = combine(v_buf, c, q)
            f_buf[q, r] = acc

            @pl.when(c < last)
            def _():
                far_first(lambda row: to_row(f_buf.at[q, r], f_buf, f_send, f_recv, q, row, c).start(), True, True, False)
                back_run(q).start()

            @pl.when(c == last)
            def _():
                far_first(lambda row: to_row(f_buf.at[q, r], f_buf, f_send, f_recv, q, row, c).start(), False, True, False)

            deliver(fwd_ref, q, acc)

        each_chunk(one)

    @pl.when(c == 0)
    def _():
        solve_forward(False)

    @pl.when(c > 0)
    def _():
        solve_forward(True)

    def wait_run(run, recv, k, q):
        remote(run.at[k, q], run.at[k, q], recv.at[k, q], recv.at[k, q], r, c).wait_recv()

    def sweep(buf, recv, first, count, step, run_in, run_recv, run_out, run_send, stage, out, send, out_recv, late):
        nxt = c + step

        def one(q):
            arrivals(buf, recv, q, True, True, False)
            acc = combine(buf, first, q)
            wait_run(run_in, run_recv, first, q)
            stage[q] = run_in[first, q] - acc
            far_first(
                lambda row: to_row(stage.at[q], out, send, out_recv, q, row, nxt).start(),
                step > 0, step < 0, True,
            )

        each_chunk(one)

        def other(i, _):
            k = first + step * i
            if late:
                @pl.when(c == 0)
                def _():
                    turn(k)

            def inner(q):
                acc = combine(buf, k, q)
                wait_run(run_in, run_recv, k, q)
                run_out[k, q] = run_in[k, q] - acc
                remote(run_out.at[k, q], run_in.at[k, q], run_send.at[k, q], run_recv.at[k, q], r, nxt).start()

            each_chunk(inner)
            return 0

        lax.fori_loop(1, count, other, 0)

    @pl.when(c == last)
    def _():
        set_upper()

    @pl.when(c < last)
    def _():
        sweep(f_buf, f_recv, c + 1, last - c, 1, rin, r_recv, rout, r_send, t_buf, v_buf, w_send, v_recv, True)
        set_upper()

    def solve_backward(buf, recv, own):
        def one(q):
            arrivals(buf, recv, q, True, False, own)
            acc = combine(buf, c, q)

            @pl.when(c > 0)
            def _():
                s_buf[q, r] = acc
                far_first(lambda row: to_row(s_buf.at[q, r], s_buf, s_send, s_recv, q, row, c).start(), True, True, False)

            deliver(sol_ref, q, acc)

        each_chunk(one)

    @pl.when(c == last)
    def _():
        solve_backward(f_buf, f_recv, False)

    @pl.when(c < last)
    def _():
        solve_backward(w_buf, w_recv, True)

    @pl.when(c > 0)
    def _():
        sweep(s_buf, s_recv, c - 1, c, -1, rbin, rb_recv, rbout, rb_send, tb_buf, w_buf, v_send, w_recv, False)

    def sent(src, send):
        remote(src, src, send, send, r, c).wait_send()

    def finish(q):
        @pl.when(c == 0)
        def _():
            far_first(lambda row: sent(chunk(rs_ref, q), v_send.at[q, row]), True, False, False)

        @pl.when(c > 0)
        def _():
            sent(chunk(rs_ref, q), r_send.at[c, q])
            far_first(lambda row: sent(tb_buf.at[q], v_send.at[q, row]), False, True, True)
            far_first(lambda row: sent(s_buf.at[q, r], s_send.at[q, row]), True, True, False)

        @pl.when(c < last)
        def _():
            far_first(lambda row: sent(f_buf.at[q, r], f_send.at[q, row]), True, True, False)
            sent(f_buf.at[q, r], b0_send.at[q])
            far_first(lambda row: sent(t_buf.at[q], w_send.at[q, row]), True, False, True)

        @pl.when(c == last)
        def _():
            far_first(lambda row: sent(f_buf.at[q, r], f_send.at[q, row]), False, True, False)

        def run(k, _):
            @pl.when(k > c + 1)
            def _():
                sent(rout.at[k, q], r_send.at[k, q])

            @pl.when(k < c - 1)
            def _():
                sent(rbout.at[k, q], rb_send.at[k, q])

            return 0

        lax.fori_loop(0, n_col, run, 0)

    each_chunk(finish)


def local(n_row, n_col, factors, right_side):
    tiles, rows, size = factors.shape
    width = right_side.shape[2]
    chunks = CHUNKS
    portion = width // chunks
    padded = -(-rows // 128) * 128

    vmem = pl.BlockSpec(memory_space=pltpu.VMEM)
    anywhere = pl.BlockSpec(memory_space=pl.ANY)
    gathered = pltpu.VMEM((chunks, n_row, portion, rows), jnp.float32)
    staged = pltpu.VMEM((chunks, portion, rows), jnp.float32)
    runs = pltpu.VMEM((tiles, chunks, portion, rows), jnp.float32)
    weights = pltpu.VMEM((tiles, n_row, rows, rows), jnp.bfloat16)
    dma = pltpu.SemaphoreType.DMA
    shape = jax.ShapeDtypeStruct((1, width, rows), jnp.float32)
    forward, backward = pl.pallas_call(
        functools.partial(kernel, n_row, n_col, chunks, rows, size, width),
        out_shape=(shape, shape),
        in_specs=[anywhere, vmem],
        out_specs=(vmem, vmem),
        scratch_shapes=[
            pltpu.VMEM((tiles, padded, size), jnp.float32), pltpu.VMEM((size, padded), jnp.float32),
            pltpu.VMEM((rows, rows), jnp.float32), weights, weights,
            gathered, gathered, gathered, gathered, staged, staged, runs, runs, runs, runs,
            dma((tiles,)),
            *([dma((chunks, n_row))] * 8),
            *([dma((tiles, chunks))] * 4),
            dma((chunks,)),
        ],
        compiler_params=pltpu.CompilerParams(collective_id=0, has_side_effects=True, vmem_limit_bytes=60 << 20),
    )(factors, right_side.transpose(0, 2, 1))
    return forward.transpose(0, 2, 1), backward.transpose(0, 2, 1)


def solution(mesh):
    return jax.shard_map(
        functools.partial(local, mesh.shape["row"], mesh.shape["col"]),
        mesh=mesh,
        in_specs=(P("groups", "row", "col"), P(("groups", "col"), "row", None)),
        out_specs=(P(("groups", "col"), "row", None), P(("groups", "col"), "row", None)),
        check_vma=False,
    )
```

```python
import functools

import jax
import jax.numpy as jnp
from jax import lax
from jax.experimental import pallas as pl
from jax.experimental.pallas import tpu as pltpu
from jax.sharding import PartitionSpec as P

MESH = pl.DeviceIdType.MESH
CHUNKS = 6
TURN = 256
LAG = 1


def kernel(
    n_row, n_col, chunks, rows, size, width, spare,
    factors_hbm, rs_ref,
    fwd_ref, sol_ref,
    raw, turned, ahi, alo, rs_buf, v_buf, f_buf, w_buf, s_buf, t_buf, tb_buf, rin, rout, rbin, rbout,
    a_sem, v_send, v_recv, f_send, f_recv, w_send, w_recv, s_send, s_recv,
    r_send, r_recv, rb_send, rb_recv, b0_send,
):
    r = lax.axis_index("row")
    c = lax.axis_index("col")
    last = n_col - 1
    portion = width // chunks
    short = n_row <= 4
    depth = rows + spare
    whole = rows // 128

    def load(k):
        return pltpu.make_async_copy(factors_hbm.at[k], raw.at[k, pl.ds(0, rows), :], a_sem.at[k, 0])

    def load_spare(k):
        src = factors_hbm.at[k, pl.ds(rows - spare, spare), :]
        return pltpu.make_async_copy(src, raw.at[k, pl.ds(rows, spare), :], a_sem.at[k, 1])

    def start_load(i, _):
        load(lax.rem(c + i, n_col)).start()
        if spare:
            load_spare(lax.rem(c + i, n_col)).start()
        return 0

    lax.fori_loop(0, n_col, start_load, 0)

    barrier = pltpu.get_barrier_semaphore()

    def greet(i, _):
        rr, cc = i // n_col, i % n_col

        @pl.when(i != r * n_col + c)
        def _():
            pl.semaphore_signal(barrier, inc=1, device_id={"row": rr, "col": cc}, device_id_type=MESH)

        return 0

    lax.fori_loop(0, n_row * n_col, greet, 0)

    def remote(src, dst, send, recv, row, col):
        return pltpu.make_async_remote_copy(
            src_ref=src, dst_ref=dst, send_sem=send, recv_sem=recv,
            device_id={"row": row, "col": col}, device_id_type=MESH,
        )

    def each_chunk(body):
        def step(q, _):
            body(q)
            return 0

        lax.fori_loop(0, chunks, step, 0)

    def each_row(body):
        def step(s, _):
            body(s)
            return 0

        lax.fori_loop(0, n_row, step, 0, unroll=short)

    def far_first(body, up, down, own):
        def step(i, _):
            d = n_row - 1 - i
            if up:
                @pl.when(r + d < n_row)
                def _():
                    body(r + d)

            if down:
                @pl.when(r - d >= 0)
                def _():
                    body(r - d)

            return 0

        lax.fori_loop(0, n_row - 1, step, 0, unroll=short)
        if own:
            body(r)

    def split(x):
        hi = x.astype(jnp.bfloat16)
        return hi, (x - hi.astype(jnp.float32)).astype(jnp.bfloat16)

    def halves(value):
        lane = lax.broadcasted_iota(jnp.int32, value.shape, 1)
        return lane < spare

    def unpack(block):
        if not spare:
            return block
        parts = [block[i * portion : (i + 1) * portion] for i in range(whole)]
        rest = block[whole * portion :]
        left = halves(rest)
        parts.append(jnp.concatenate([jnp.where(left, rest, 0.0), jnp.where(left, 0.0, rest)], axis=0))
        return jnp.concatenate(parts, axis=1)

    def pack(value):
        if not spare:
            return value
        parts = [value[:, i * 128 : (i + 1) * 128] for i in range(whole)]
        rest = value[:, whole * 128 :]
        top, low = rest[: portion // 2], rest[portion // 2 :]
        return jnp.concatenate([*parts, jnp.where(halves(top), top, low)], axis=0)

    def combine(buf, index, q):
        def step(s, acc):
            hi, lo = split(unpack(buf[q, s]))
            both = jnp.concatenate([hi, lo], axis=0)
            one = jnp.dot(both, ahi[index(s)], preferred_element_type=jnp.float32)
            two = jnp.dot(hi, alo[index(s)], preferred_element_type=jnp.float32)
            return acc + (one[:portion] + one[portion:] + two)

        zero = jnp.zeros((portion, depth), jnp.float32)
        return lax.fori_loop(0, n_row, step, zero, unroll=short)

    def tile(k):
        return lambda s: k * n_row + s

    def upper(s):
        same = 1 // (1 + (s - r) * (s - r))
        return c * n_row + s + same * ((n_col - c) * n_row - s)

    def arrive(buf, recv, q, s):
        remote(buf.at[q, s], buf.at[q, s], recv.at[q, s], recv.at[q, s], r, c).wait_recv()

    def arrivals(buf, recv, q, up, down, own):
        def one(s):
            wanted = None if own else s != r
            if not up:
                wanted = s <= r if own else s < r
            if not down:
                wanted = s >= r if own else s > r
            if wanted is None:
                arrive(buf, recv, q, s)
            else:
                @pl.when(wanted)
                def _():
                    arrive(buf, recv, q, s)

        each_row(one)

    def to_row(src, buf, send, recv, q, row, col):
        return remote(src, buf.at[q, r], send.at[q, row], recv.at[q, r], row, col)

    def prepare(q):
        value = rs_ref[0, pl.ds(pl.multiple_of(q * portion, 8), portion), :]
        if spare:
            value = jnp.concatenate([value, value[:, rows - spare :]], axis=1)
        rs_buf[q] = pack(value)

        @pl.when(c == 0)
        def _():
            v_buf[q, r] = rs_buf[q]

    each_chunk(prepare)

    def blank(s):
        zero = jnp.zeros((chunks, *v_buf.shape[2:]), jnp.float32)

        @pl.when(s > r)
        def _():
            v_buf[:, s] = zero

        @pl.when(s < r)
        def _():
            w_buf[:, s] = zero

            @pl.when(c == last)
            def _():
                f_buf[:, s] = zero

    each_row(blank)

    def store(at, value):
        hi, lo = split(value)
        ahi[at, pl.ds(0, rows), :] = hi
        alo[at, pl.ds(0, rows), :] = lo
        if spare:
            ahi[at, pl.ds(rows, spare), :] = hi[rows - spare :]
            alo[at, pl.ds(rows, spare), :] = lo[rows - spare :]

    def band(s):
        return turned[pl.ds(pl.multiple_of(s * rows, 8), rows), :depth]

    def turn(k):
        def step(j, _):
            base = pl.multiple_of(j * TURN, TURN)
            turned[pl.ds(base, TURN), :] = raw[k, :, pl.ds(base, TURN)].T
            return 0

        load(k).wait()
        if spare:
            load_spare(k).wait()
        lax.fori_loop(0, size // TURN, step, 0)

        def cut(s, _):
            store(k * n_row + s, band(s))
            return 0

        lax.fori_loop(0, n_row, cut, 0)

    def corners():
        column = lax.broadcasted_iota(jnp.int32, (rows, depth), 0)
        line = lax.broadcasted_iota(jnp.int32, (rows, depth), 1)
        line = line - jnp.where(line >= rows, spare, 0)
        value = band(r)
        store(c * n_row + r, jnp.where(column < line, value, jnp.where(column == line, 1.0, 0.0)))
        store(n_col * n_row, jnp.where(column >= line, value, 0.0))

    turn(c)
    corners()
    pl.semaphore_wait(barrier, n_row * n_col - 1)

    @pl.when(c == 0)
    def _():
        def one(q):
            far_first(lambda row: to_row(rs_buf.at[q], v_buf, v_send, v_recv, q, row, c).start(), True, False, False)

        each_chunk(one)

    def first_run(q):
        return remote(rs_buf.at[q], rin.at[c, q], r_send.at[c, q], r_recv.at[c, q], r, 0)

    @pl.when(c > 0)
    def _():
        each_chunk(lambda q: first_run(q).start())

    def turn_others(i, _):
        turn(lax.rem(c + i, n_col))
        return 0

    lax.fori_loop(1, n_col, turn_others, 0)

    def back_run(q):
        return remote(f_buf.at[q, r], rbin.at[c, q], b0_send.at[q], rb_recv.at[c, q], r, last)

    def deliver(ref, q, value):
        ref[0, pl.ds(pl.multiple_of(q * portion, 8), portion), :] = value[:, :rows]

    def forward_of(own, is_last):
        def one(q):
            arrivals(v_buf, v_recv, q, False, True, own)
            acc = combine(v_buf, tile(c), q)
            f_buf[q, r] = pack(acc)
            far_first(
                lambda row: to_row(f_buf.at[q, r], f_buf, f_send, f_recv, q, row, c).start(), not is_last, True, False
            )
            if not is_last:
                back_run(q).start()
            deliver(fwd_ref, q, acc)

        return one

    def wait_run(run, recv, k, q):
        remote(run.at[k, q], run.at[k, q], recv.at[k, q], recv.at[k, q], r, c).wait_recv()

    def sweep_of(buf, recv, count, step, run_in, run_recv, run_out, run_send, stage, out, send, out_recv):
        nxt = c + step

        def one(q):
            arrivals(buf, recv, q, True, True, False)
            acc = combine(buf, tile(nxt), q)
            wait_run(run_in, run_recv, nxt, q)
            stage[q] = run_in[nxt, q] - pack(acc)
            far_first(
                lambda row: to_row(stage.at[q], out, send, out_recv, q, row, nxt).start(),
                step > 0, step < 0, True,
            )

            def other(i, _):
                k = nxt + step * i
                acc = combine(buf, tile(k), q)
                wait_run(run_in, run_recv, k, q)
                run_out[k, q] = run_in[k, q] - pack(acc)
                remote(run_out.at[k, q], run_in.at[k, q], run_send.at[k, q], run_recv.at[k, q], r, nxt).start()
                return 0

            lax.fori_loop(1, count, other, 0)

        return one

    def backward_of(buf, recv, own, is_first):
        def one(q):
            arrivals(buf, recv, q, True, False, own)
            acc = combine(buf, upper, q)
            if not is_first:
                s_buf[q, r] = pack(acc)
                far_first(lambda row: to_row(s_buf.at[q, r], s_buf, s_send, s_recv, q, row, c).start(), True, True, False)
            deliver(sol_ref, q, acc)

        return one

    def pipeline(*bodies):
        def step(t, _):
            for i, body in enumerate(bodies):
                @pl.when((t >= i * LAG) & (t < i * LAG + chunks))
                def _():
                    body(t - i * LAG)

            return 0

        lax.fori_loop(0, chunks + (len(bodies) - 1) * LAG, step, 0)

    down = sweep_of(f_buf, f_recv, last - c, 1, rin, r_recv, rout, r_send, t_buf, v_buf, w_send, v_recv)
    back = sweep_of(s_buf, s_recv, c, -1, rbin, rb_recv, rbout, rb_send, tb_buf, w_buf, v_send, w_recv)

    @pl.when(c == 0)
    def _():
        pipeline(forward_of(False, False), down)
        pipeline(backward_of(w_buf, w_recv, True, True))

    @pl.when((c > 0) & (c < last))
    def _():
        pipeline(forward_of(True, False), down)
        pipeline(backward_of(w_buf, w_recv, True, False), back)

    @pl.when(c == last)
    def _():
        pipeline(forward_of(True, True), backward_of(f_buf, f_recv, False, False), back)

    def sent(src, send):
        remote(src, src, send, send, r, c).wait_send()

    def finish(q):
        @pl.when(c == 0)
        def _():
            far_first(lambda row: sent(rs_buf.at[q], v_send.at[q, row]), True, False, False)

        @pl.when(c > 0)
        def _():
            sent(rs_buf.at[q], r_send.at[c, q])
            far_first(lambda row: sent(tb_buf.at[q], v_send.at[q, row]), False, True, True)
            far_first(lambda row: sent(s_buf.at[q, r], s_send.at[q, row]), True, True, False)

        @pl.when(c < last)
        def _():
            far_first(lambda row: sent(f_buf.at[q, r], f_send.at[q, row]), True, True, False)
            sent(f_buf.at[q, r], b0_send.at[q])
            far_first(lambda row: sent(t_buf.at[q], w_send.at[q, row]), True, False, True)

        @pl.when(c == last)
        def _():
            far_first(lambda row: sent(f_buf.at[q, r], f_send.at[q, row]), False, True, False)

        def run(k, _):
            @pl.when(k > c + 1)
            def _():
                sent(rout.at[k, q], r_send.at[k, q])

            @pl.when(k < c - 1)
            def _():
                sent(rbout.at[k, q], rb_send.at[k, q])

            return 0

        lax.fori_loop(0, n_col, run, 0)

    each_chunk(finish)


def local(n_row, n_col, factors, right_side):
    tiles, rows, size = factors.shape
    width = right_side.shape[2]
    chunks = CHUNKS
    portion = width // chunks
    spare = 64 if rows % 128 == 64 and portion % 16 == 0 else 0
    padded = -(-rows // 128) * 128
    depth = rows + spare

    vmem = pl.BlockSpec(memory_space=pltpu.VMEM)
    anywhere = pl.BlockSpec(memory_space=pl.ANY)
    block = (portion * depth // 128 - spare * portion // 128, 128) if spare else (portion, rows)
    gathered = pltpu.VMEM((chunks, n_row, *block), jnp.float32)
    staged = pltpu.VMEM((chunks, *block), jnp.float32)
    runs = pltpu.VMEM((tiles, chunks, *block), jnp.float32)
    weights = pltpu.VMEM((tiles * n_row + 1, depth, depth), jnp.bfloat16)
    dma = pltpu.SemaphoreType.DMA
    shape = jax.ShapeDtypeStruct((1, width, rows), jnp.float32)
    forward, backward = pl.pallas_call(
        functools.partial(kernel, n_row, n_col, chunks, rows, size, width, spare),
        out_shape=(shape, shape),
        in_specs=[anywhere, vmem],
        out_specs=(vmem, vmem),
        scratch_shapes=[
            pltpu.VMEM((tiles, padded, size), jnp.float32), pltpu.VMEM((size, padded), jnp.float32),
            weights, weights, staged,
            gathered, gathered, gathered, gathered, staged, staged, runs, runs, runs, runs,
            dma((tiles, 2)),
            *([dma((chunks, n_row))] * 8),
            *([dma((tiles, chunks))] * 4),
            dma((chunks,)),
        ],
        compiler_params=pltpu.CompilerParams(collective_id=0, has_side_effects=True, vmem_limit_bytes=60 << 20),
    )(factors, right_side.transpose(0, 2, 1))
    return forward.transpose(0, 2, 1), backward.transpose(0, 2, 1)


def solution(mesh):
    return jax.shard_map(
        functools.partial(local, mesh.shape["row"], mesh.shape["col"]),
        mesh=mesh,
        in_specs=(P("groups", "row", "col"), P(("groups", "col"), "row", None)),
        out_specs=(P(("groups", "col"), "row", None), P(("groups", "col"), "row", None)),
        check_vma=False,
    )
```

```python
import functools

import jax
import jax.numpy as jnp
from jax import lax
from jax.experimental import pallas as pl
from jax.experimental.pallas import tpu as pltpu
from jax.sharding import PartitionSpec as P

MESH = pl.DeviceIdType.MESH
CHUNKS = 6
TURN = 256
GROUPS = 2
DELAY = 3


def kernel(
    n_row, n_col, chunks, rows, size, width, spare,
    factors_hbm, rs_ref,
    fwd_ref, sol_ref,
    raw, turned, ahi, alo, rs_buf, v_buf, f_buf, w_buf, s_buf, t_buf, tb_buf, rin, rout, rbin, rbout,
    a_sem, v_send, v_recv, f_send, f_recv, w_send, w_recv, s_send, s_recv,
    r_send, r_recv, rb_send, rb_recv, b0_send, g_send,
):
    r = lax.axis_index("row")
    c = lax.axis_index("col")
    last = n_col - 1
    portion = width // chunks
    short = n_row <= 4
    depth = rows + spare
    whole = rows // 128

    def load(k):
        return pltpu.make_async_copy(factors_hbm.at[k], raw.at[k, pl.ds(0, rows), :], a_sem.at[k, 0])

    def load_spare(k):
        src = factors_hbm.at[k, pl.ds(rows - spare, spare), :]
        return pltpu.make_async_copy(src, raw.at[k, pl.ds(rows, spare), :], a_sem.at[k, 1])

    def start_load(i, _):
        load(lax.rem(c + i, n_col)).start()
        if spare:
            load_spare(lax.rem(c + i, n_col)).start()
        return 0

    lax.fori_loop(0, n_col, start_load, 0)

    barrier = pltpu.get_barrier_semaphore()

    def greet(i, _):
        rr, cc = i // n_col, i % n_col

        @pl.when(i != r * n_col + c)
        def _():
            pl.semaphore_signal(barrier, inc=1, device_id={"row": rr, "col": cc}, device_id_type=MESH)

        return 0

    lax.fori_loop(0, n_row * n_col, greet, 0)

    def remote(src, dst, send, recv, row, col):
        return pltpu.make_async_remote_copy(
            src_ref=src, dst_ref=dst, send_sem=send, recv_sem=recv,
            device_id={"row": row, "col": col}, device_id_type=MESH,
        )

    def each_chunk(body):
        def step(q, _):
            body(q)
            return 0

        lax.fori_loop(0, chunks, step, 0)

    def each_row(body):
        def step(s, _):
            body(s)
            return 0

        lax.fori_loop(0, n_row, step, 0, unroll=short)

    def far_first(body, up, down, own, top=None, bottom=None):
        def step(i, _):
            d = n_row - 1 - i
            if down:
                @pl.when(r - d >= (0 if bottom is None else bottom))
                def _():
                    body(r - d)

            if up:
                @pl.when(r + d <= (n_row - 1 if top is None else top))
                def _():
                    body(r + d)

            return 0

        lax.fori_loop(0, n_row - 1, step, 0, unroll=short)
        if own:
            body(r)

    relays = g_send.shape[1] > 1
    half = n_row // 2
    mirror = n_row - 1 - half

    def spread(body, ahead):
        if not relays:
            far_first(body, True, True, False)
        elif ahead:
            @pl.when(r < half)
            def _():
                far_first(body, True, True, False, top=half)

            @pl.when(r >= half)
            def _():
                far_first(body, True, True, False)
        else:
            @pl.when(r > mirror)
            def _():
                far_first(body, True, True, False, bottom=mirror)

            @pl.when(r <= mirror)
            def _():
                far_first(body, True, True, False)

    def relayed(body, ahead):
        if not relays:
            return
        if ahead:
            @pl.when(r == half)
            def _():
                for s in range(half):
                    for row in range(half + 1, n_row):
                        body(s, row, row - half - 1)
        else:
            @pl.when(r == mirror)
            def _():
                for s in range(n_row - 1, mirror, -1):
                    for row in range(mirror):
                        body(s, row, row)

    def split(x):
        hi = x.astype(jnp.bfloat16)
        return hi, (x - hi.astype(jnp.float32)).astype(jnp.bfloat16)

    def halves(value):
        lane = lax.broadcasted_iota(jnp.int32, value.shape, 1)
        return lane < spare

    def unpack(block):
        if not spare:
            return block
        parts = [block[i * portion : (i + 1) * portion] for i in range(whole)]
        rest = block[whole * portion :]
        left = halves(rest)
        parts.append(jnp.concatenate([jnp.where(left, rest, 0.0), jnp.where(left, 0.0, rest)], axis=0))
        return jnp.concatenate(parts, axis=1)

    def pack(value):
        if not spare:
            return value
        parts = [value[:, i * 128 : (i + 1) * 128] for i in range(whole)]
        rest = value[:, whole * 128 :]
        top, low = rest[: portion // 2], rest[portion // 2 :]
        return jnp.concatenate([*parts, jnp.where(halves(top), top, low)], axis=0)

    def combine(buf, index, q, count=1):
        portion = width // chunks * count

        def step(s, acc):
            hi, lo = split(jnp.concatenate([unpack(buf[q + i, s]) for i in range(count)], axis=0))
            both = jnp.concatenate([hi, lo], axis=0)
            one = jnp.dot(both, ahi[index(s)], preferred_element_type=jnp.float32)
            two = jnp.dot(hi, alo[index(s)], preferred_element_type=jnp.float32)
            return acc + (one[:portion] + one[portion:] + two)

        zero = jnp.zeros((portion, depth), jnp.float32)
        return lax.fori_loop(0, n_row, step, zero, unroll=short)

    def tile(k):
        return lambda s: k * n_row + s

    def upper(s):
        same = 1 // (1 + (s - r) * (s - r))
        return c * n_row + s + same * ((n_col - c) * n_row - s)

    def arrive(buf, recv, q, s):
        remote(buf.at[q, s], buf.at[q, s], recv.at[q, s], recv.at[q, s], r, c).wait_recv()

    def arrivals(buf, recv, q, up, down, own):
        def one(s):
            wanted = None if own else s != r
            if not up:
                wanted = s <= r if own else s < r
            if not down:
                wanted = s >= r if own else s > r
            if wanted is None:
                arrive(buf, recv, q, s)
            else:
                @pl.when(wanted)
                def _():
                    arrive(buf, recv, q, s)

        each_row(one)

    def gather(buf, recv, q, ahead):
        def one(i):
            s = i if ahead else n_row - 1 - i
            wanted = s != r
            if relays and ahead:
                wanted = wanted & ((r != half) | (s > half))
            if relays and not ahead:
                wanted = wanted & ((r != mirror) | (s < mirror))

            @pl.when(wanted)
            def _():
                arrive(buf, recv, q, s)

        each_row(one)

    def relay(buf, recv, q, s, row, slot):
        return remote(buf.at[q, s], buf.at[q, s], g_send.at[q, s, slot], recv.at[q, s], row, c)

    def pass_on_of(buf, recv, ahead):
        def one(q):
            def step(s, row, slot):
                if slot == 0:
                    arrive(buf, recv, q, s)
                relay(buf, recv, q, s, row, slot).start()

            relayed(step, ahead)

        return one

    def to_row(src, buf, send, recv, q, row, col):
        return remote(src, buf.at[q, r], send.at[q, row], recv.at[q, r], row, col)

    def prepare(q):
        value = rs_ref[0, pl.ds(pl.multiple_of(q * portion, 8), portion), :]
        if spare:
            value = jnp.concatenate([value, value[:, rows - spare :]], axis=1)
        rs_buf[q] = pack(value)

        @pl.when(c == 0)
        def _():
            v_buf[q, r] = rs_buf[q]

    each_chunk(prepare)

    def blank(s):
        zero = jnp.zeros((chunks, *v_buf.shape[2:]), jnp.float32)

        @pl.when(s > r)
        def _():
            v_buf[:, s] = zero

        @pl.when(s < r)
        def _():
            w_buf[:, s] = zero

            @pl.when(c == last)
            def _():
                f_buf[:, s] = zero

    each_row(blank)

    def store(at, value):
        hi, lo = split(value)
        ahi[at, pl.ds(0, rows), :] = hi
        alo[at, pl.ds(0, rows), :] = lo
        if spare:
            ahi[at, pl.ds(rows, spare), :] = hi[rows - spare :]
            alo[at, pl.ds(rows, spare), :] = lo[rows - spare :]

    def band(s):
        return turned[pl.ds(pl.multiple_of(s * rows, 8), rows), :depth]

    def turn(k):
        def step(j, _):
            base = pl.multiple_of(j * TURN, TURN)
            turned[pl.ds(base, TURN), :] = raw[k, :, pl.ds(base, TURN)].T
            return 0

        load(k).wait()
        if spare:
            load_spare(k).wait()
        lax.fori_loop(0, size // TURN, step, 0)

        def cut(s, _):
            store(k * n_row + s, band(s))
            return 0

        lax.fori_loop(0, n_row, cut, 0)

    def corners():
        column = lax.broadcasted_iota(jnp.int32, (rows, depth), 0)
        line = lax.broadcasted_iota(jnp.int32, (rows, depth), 1)
        line = line - jnp.where(line >= rows, spare, 0)
        value = band(r)
        store(c * n_row + r, jnp.where(column < line, value, jnp.where(column == line, 1.0, 0.0)))
        store(n_col * n_row, jnp.where(column >= line, value, 0.0))

    turn(c)
    corners()
    pl.semaphore_wait(barrier, n_row * n_col - 1)

    def enter(q):
        far_first(lambda row: to_row(rs_buf.at[q], v_buf, v_send, v_recv, q, row, c).start(), True, False, False)

    def each_of(g, body):
        def step(i, _):
            body(g * (chunks // GROUPS) + i)
            return 0

        lax.fori_loop(0, chunks // GROUPS, step, 0)

    @pl.when(c == 0)
    def _():
        each_of(0, enter)

    def first_run(q):
        return remote(rs_buf.at[q], rin.at[c, q], r_send.at[c, q], r_recv.at[c, q], r, 0)

    @pl.when(c > 0)
    def _():
        each_chunk(lambda q: first_run(q).start())

    def turn_others(i, _):
        turn(lax.rem(c + i, n_col))
        return 0

    lax.fori_loop(1, n_col, turn_others, 0)

    def back_run(q):
        return remote(f_buf.at[q, r], rbin.at[c, q], b0_send.at[q], rb_recv.at[c, q], r, last)

    def deliver(ref, q, value):
        ref[0, pl.ds(pl.multiple_of(q * portion, 8), portion), :] = value[:, :rows]

    def forward_of(own, is_last):
        def one(q):
            arrivals(v_buf, v_recv, q, False, True, own)
            acc = combine(v_buf, tile(c), q)
            f_buf[q, r] = pack(acc)
            if is_last:
                far_first(lambda row: to_row(f_buf.at[q, r], f_buf, f_send, f_recv, q, row, c).start(), False, True, False)
            else:
                spread(lambda row: to_row(f_buf.at[q, r], f_buf, f_send, f_recv, q, row, c).start(), True)
                back_run(q).start()
            deliver(fwd_ref, q, acc)

        return one

    def wait_run(run, recv, k, q):
        remote(run.at[k, q], run.at[k, q], recv.at[k, q], recv.at[k, q], r, c).wait_recv()

    def sweep_of(buf, recv, count, step, run_in, run_recv, run_out, run_send, stage, out, send, out_recv):
        nxt = c + step

        def one(q):
            gather(buf, recv, q, step > 0)
            acc = combine(buf, tile(nxt), q)
            wait_run(run_in, run_recv, nxt, q)
            stage[q] = run_in[nxt, q] - pack(acc)
            far_first(
                lambda row: to_row(stage.at[q], out, send, out_recv, q, row, nxt).start(),
                step > 0, step < 0, True,
            )

        def rest(g):
            each = chunks // GROUPS

            def other(i, _):
                k = nxt + step * i
                acc = combine(buf, tile(k), g * each, each)
                for part in range(each):
                    q = g * each + part
                    wait_run(run_in, run_recv, k, q)
                    run_out[k, q] = run_in[k, q] - pack(acc[part * portion : (part + 1) * portion])
                    remote(run_out.at[k, q], run_in.at[k, q], run_send.at[k, q], run_recv.at[k, q], r, nxt).start()
                return 0

            lax.fori_loop(1, count, other, 0)

        return one, rest

    def backward_of(buf, recv, own, is_first):
        def one(q):
            arrivals(buf, recv, q, True, False, own)
            acc = combine(buf, upper, q)
            if not is_first:
                s_buf[q, r] = pack(acc)
                spread(lambda row: to_row(s_buf.at[q, r], s_buf, s_send, s_recv, q, row, c).start(), False)
            deliver(sol_ref, q, acc)

        return one

    def pipeline(final, *stages):
        def step(t, _):
            for first, body in stages:
                @pl.when((t >= first) & (t < first + DELAY * GROUPS) & ((t + DELAY - first % DELAY) % DELAY == 0))
                def _():
                    if body in (down_rest, back_rest):
                        body((t - first) // DELAY)
                    else:
                        each_of((t - first) // DELAY, body)

            return 0

        lax.fori_loop(0, final + DELAY * (GROUPS - 1) + 1, step, 0)

    down, down_rest = sweep_of(f_buf, f_recv, last - c, 1, rin, r_recv, rout, r_send, t_buf, v_buf, w_send, v_recv)
    back, back_rest = sweep_of(s_buf, s_recv, c, -1, rbin, rb_recv, rbout, rb_send, tb_buf, w_buf, v_send, w_recv)

    pass_down = pass_on_of(f_buf, f_recv, True)
    pass_back = pass_on_of(s_buf, s_recv, False)

    @pl.when(c == 0)
    def _():
        def enter_next(q):
            @pl.when(q + chunks // GROUPS < chunks)
            def _():
                enter(q + chunks // GROUPS)

        pipeline(
            4 * last + 1,
            (1, pass_down), (1, down), (0, forward_of(False, False)), (DELAY - 1, enter_next), (1, down_rest),
            (4 * last + 1, backward_of(w_buf, w_recv, True, True)),
        )

    @pl.when((c > 0) & (c < last))
    def _():
        turned_back = 4 * (last - c) + 1
        pipeline(
            turned_back + 1,
            (turned_back + 1, pass_back), (turned_back + 1, back), (turned_back, backward_of(w_buf, w_recv, True, False)),
            (1, pass_down), (1, down), (0, forward_of(True, False)),
            (1, down_rest), (turned_back + 1, back_rest),
        )

    @pl.when(c == last)
    def _():
        pipeline(
            2,
            (2, pass_back), (2, back), (1, backward_of(f_buf, f_recv, False, False)), (0, forward_of(True, True)),
            (2, back_rest),
        )

    def sent(src, send):
        remote(src, src, send, send, r, c).wait_send()

    def finish(q):
        @pl.when(c == 0)
        def _():
            far_first(lambda row: sent(rs_buf.at[q], v_send.at[q, row]), True, False, False)

        @pl.when(c > 0)
        def _():
            sent(rs_buf.at[q], r_send.at[c, q])
            far_first(lambda row: sent(tb_buf.at[q], v_send.at[q, row]), False, True, True)
            spread(lambda row: sent(s_buf.at[q, r], s_send.at[q, row]), False)
            relayed(lambda s, row, slot: sent(s_buf.at[q, s], g_send.at[q, s, slot]), False)

        @pl.when(c < last)
        def _():
            spread(lambda row: sent(f_buf.at[q, r], f_send.at[q, row]), True)
            relayed(lambda s, row, slot: sent(f_buf.at[q, s], g_send.at[q, s, slot]), True)
            sent(f_buf.at[q, r], b0_send.at[q])
            far_first(lambda row: sent(t_buf.at[q], w_send.at[q, row]), True, False, True)

        @pl.when(c == last)
        def _():
            far_first(lambda row: sent(f_buf.at[q, r], f_send.at[q, row]), False, True, False)

        def run(k, _):
            @pl.when(k > c + 1)
            def _():
                sent(rout.at[k, q], r_send.at[k, q])

            @pl.when(k < c - 1)
            def _():
                sent(rbout.at[k, q], rb_send.at[k, q])

            return 0

        lax.fori_loop(0, n_col, run, 0)

    each_chunk(finish)


def local(n_row, n_col, factors, right_side):
    tiles, rows, size = factors.shape
    width = right_side.shape[2]
    chunks = CHUNKS
    portion = width // chunks
    spare = 64 if rows % 128 == 64 and portion % 16 == 0 else 0
    padded = -(-rows // 128) * 128
    depth = rows + spare

    vmem = pl.BlockSpec(memory_space=pltpu.VMEM)
    anywhere = pl.BlockSpec(memory_space=pl.ANY)
    block = (portion * depth // 128 - spare * portion // 128, 128) if spare else (portion, rows)
    gathered = pltpu.VMEM((chunks, n_row, *block), jnp.float32)
    staged = pltpu.VMEM((chunks, *block), jnp.float32)
    runs = pltpu.VMEM((tiles, chunks, *block), jnp.float32)
    weights = pltpu.VMEM((tiles * n_row + 1, depth, depth), jnp.bfloat16)
    dma = pltpu.SemaphoreType.DMA
    shape = jax.ShapeDtypeStruct((1, width, rows), jnp.float32)
    forward, backward = pl.pallas_call(
        functools.partial(kernel, n_row, n_col, chunks, rows, size, width, spare),
        out_shape=(shape, shape),
        in_specs=[anywhere, vmem],
        out_specs=(vmem, vmem),
        scratch_shapes=[
            pltpu.VMEM((tiles, padded, size), jnp.float32), pltpu.VMEM((size, padded), jnp.float32),
            weights, weights, staged,
            gathered, gathered, gathered, gathered, staged, staged, runs, runs, runs, runs,
            dma((tiles, 2)),
            *([dma((chunks, n_row))] * 8),
            *([dma((tiles, chunks))] * 4),
            dma((chunks,)), dma((chunks, n_row, n_row // 2) if 2 < n_row <= 8 else (1, 1, 1)),
        ],
        compiler_params=pltpu.CompilerParams(collective_id=0, has_side_effects=True, vmem_limit_bytes=60 << 20),
    )(factors, right_side.transpose(0, 2, 1))
    return forward.transpose(0, 2, 1), backward.transpose(0, 2, 1)


def solution(mesh):
    return jax.shard_map(
        functools.partial(local, mesh.shape["row"], mesh.shape["col"]),
        mesh=mesh,
        in_specs=(P("groups", "row", "col"), P(("groups", "col"), "row", None)),
        out_specs=(P(("groups", "col"), "row", None), P(("groups", "col"), "row", None)),
        check_vma=False,
    )
```

```python
import functools

import jax
import jax.numpy as jnp
from jax import lax
from jax.experimental import pallas as pl
from jax.experimental.pallas import tpu as pltpu
from jax.sharding import PartitionSpec as P

MESH = pl.DeviceIdType.MESH
CHUNKS = 6
TURN = 256
GROUPS = 2
DELAY = 3


def kernel(
    n_row, n_col, chunks, rows, size, width, spare,
    factors_hbm, rs_ref,
    fwd_ref, sol_ref,
    raw, turned, ahi, alo, rs_buf, v_buf, f_buf, w_buf, s_buf, t_buf, tb_buf, rin, rout, rbin, rbout,
    a_sem, v_send, v_recv, f_send, f_recv, w_send, w_recv, s_send, s_recv,
    r_send, r_recv, rb_send, rb_recv, b0_send, g_send,
):
    r = lax.axis_index("row")
    c = lax.axis_index("col")
    last = n_col - 1
    portion = width // chunks
    short = n_row <= 4
    depth = rows + spare
    whole = rows // 128

    def load(k):
        return pltpu.make_async_copy(factors_hbm.at[k], raw.at[k, pl.ds(0, rows), :], a_sem.at[k, 0])

    def load_spare(k):
        src = factors_hbm.at[k, pl.ds(rows - spare, spare), :]
        return pltpu.make_async_copy(src, raw.at[k, pl.ds(rows, spare), :], a_sem.at[k, 1])

    def start_load(i, _):
        load(lax.rem(c + i, n_col)).start()
        if spare:
            load_spare(lax.rem(c + i, n_col)).start()
        return 0

    lax.fori_loop(0, n_col, start_load, 0)

    barrier = pltpu.get_barrier_semaphore()

    def greet(i, _):
        rr, cc = i // n_col, i % n_col

        @pl.when(i != r * n_col + c)
        def _():
            pl.semaphore_signal(barrier, inc=1, device_id={"row": rr, "col": cc}, device_id_type=MESH)

        return 0

    lax.fori_loop(0, n_row * n_col, greet, 0)

    def remote(src, dst, send, recv, row, col):
        return pltpu.make_async_remote_copy(
            src_ref=src, dst_ref=dst, send_sem=send, recv_sem=recv,
            device_id={"row": row, "col": col}, device_id_type=MESH,
        )

    def each_chunk(body):
        def step(q, _):
            body(q)
            return 0

        lax.fori_loop(0, chunks, step, 0)

    def each_row(body, first=0, stop=n_row):
        def step(s, _):
            body(s)
            return 0

        lax.fori_loop(first, stop, step, 0, unroll=short)

    def far_first(body, up, down, own, top=None, bottom=None):
        def step(i, _):
            d = n_row - 1 - i
            if down:
                @pl.when(r - d >= (0 if bottom is None else bottom))
                def _():
                    body(r - d)

            if up:
                @pl.when(r + d <= (n_row - 1 if top is None else top))
                def _():
                    body(r + d)

            return 0

        lax.fori_loop(0, n_row - 1, step, 0, unroll=short)
        if own:
            body(r)

    relays = g_send.shape[1] > 1
    half = n_row // 2
    mirror = n_row - 1 - half

    def spread(body, ahead):
        if not relays:
            far_first(body, True, True, False)
        elif ahead:
            @pl.when(r < half)
            def _():
                far_first(body, True, True, False, top=half)

            @pl.when(r >= half)
            def _():
                far_first(body, True, True, False)
        else:
            @pl.when(r > mirror)
            def _():
                far_first(body, True, True, False, bottom=mirror)

            @pl.when(r <= mirror)
            def _():
                far_first(body, True, True, False)

    def relayed(body, ahead):
        if not relays:
            return
        if ahead:
            @pl.when(r == half)
            def _():
                for s in range(half):
                    for row in range(half + 1, n_row):
                        body(s, row, row - half - 1)
        else:
            @pl.when(r == mirror)
            def _():
                for s in range(n_row - 1, mirror, -1):
                    for row in range(mirror):
                        body(s, row, row)

    def split(x):
        hi = x.astype(jnp.bfloat16)
        return hi, (x - hi.astype(jnp.float32)).astype(jnp.bfloat16)

    def halves(value):
        lane = lax.broadcasted_iota(jnp.int32, value.shape, 1)
        return lane < spare

    def unpack(block):
        if not spare:
            return block
        parts = [block[i * portion : (i + 1) * portion] for i in range(whole)]
        rest = block[whole * portion :]
        left = halves(rest)
        parts.append(jnp.concatenate([jnp.where(left, rest, 0.0), jnp.where(left, 0.0, rest)], axis=0))
        return jnp.concatenate(parts, axis=1)

    def pack(value):
        if not spare:
            return value
        parts = [value[:, i * 128 : (i + 1) * 128] for i in range(whole)]
        rest = value[:, whole * 128 :]
        top, low = rest[: portion // 2], rest[portion // 2 :]
        return jnp.concatenate([*parts, jnp.where(halves(top), top, low)], axis=0)

    def combine(buf, index, q, count=1, first=0, stop=n_row, start=None):
        portion = width // chunks * count

        def step(s, acc):
            hi, lo = split(jnp.concatenate([unpack(buf[q + i, s]) for i in range(count)], axis=0))
            both = jnp.concatenate([hi, lo], axis=0)
            one = jnp.dot(both, ahi[index(s)], preferred_element_type=jnp.float32)
            two = jnp.dot(hi, alo[index(s)], preferred_element_type=jnp.float32)
            return acc + (one[:portion] + one[portion:] + two)

        if start is None:
            start = jnp.zeros((portion, depth), jnp.float32)
        return lax.fori_loop(first, stop, step, start, unroll=short)

    def combine_as_they_come(buf, index, q, wait, last_row):
        others = (1, n_row) if last_row == 0 else (0, n_row - 1)
        final = (last_row, last_row + 1)
        wait(*others)
        acc = combine(buf, index, q, 1, *others)
        wait(*final)
        return combine(buf, index, q, 1, *final, acc)

    def tile(k):
        return lambda s: k * n_row + s

    def upper(s):
        same = 1 // (1 + (s - r) * (s - r))
        return c * n_row + s + same * ((n_col - c) * n_row - s)

    def arrive(buf, recv, q, s):
        remote(buf.at[q, s], buf.at[q, s], recv.at[q, s], recv.at[q, s], r, c).wait_recv()

    def arrivals(buf, recv, q, up, down, own, first, stop):
        def one(s):
            wanted = None if own else s != r
            if not up:
                wanted = s <= r if own else s < r
            if not down:
                wanted = s >= r if own else s > r
            if wanted is None:
                arrive(buf, recv, q, s)
            else:
                @pl.when(wanted)
                def _():
                    arrive(buf, recv, q, s)

        each_row(one, first, stop)

    def gather(buf, recv, q, ahead, first, stop):
        def one(i):
            s = i if ahead else first + stop - 1 - i
            wanted = s != r
            if relays and ahead:
                wanted = wanted & ((r != half) | (s > half))
            if relays and not ahead:
                wanted = wanted & ((r != mirror) | (s < mirror))

            @pl.when(wanted)
            def _():
                arrive(buf, recv, q, s)

        each_row(one, first, stop)

    def relay(buf, recv, q, s, row, slot):
        return remote(buf.at[q, s], buf.at[q, s], g_send.at[q, s, slot], recv.at[q, s], row, c)

    def pass_on_of(buf, recv, ahead):
        def one(q):
            def step(s, row, slot):
                if slot == 0:
                    arrive(buf, recv, q, s)
                relay(buf, recv, q, s, row, slot).start()

            relayed(step, ahead)

        return one

    def to_row(src, buf, send, recv, q, row, col):
        return remote(src, buf.at[q, r], send.at[q, row], recv.at[q, r], row, col)

    def prepare(q):
        value = rs_ref[0, pl.ds(pl.multiple_of(q * portion, 8), portion), :]
        if spare:
            value = jnp.concatenate([value, value[:, rows - spare :]], axis=1)
        rs_buf[q] = pack(value)

        @pl.when(c == 0)
        def _():
            v_buf[q, r] = rs_buf[q]

    each_chunk(prepare)

    def blank(s):
        zero = jnp.zeros((chunks, *v_buf.shape[2:]), jnp.float32)

        @pl.when(s > r)
        def _():
            v_buf[:, s] = zero

        @pl.when(s < r)
        def _():
            w_buf[:, s] = zero

            @pl.when(c == last)
            def _():
                f_buf[:, s] = zero

    each_row(blank)

    def store(at, value):
        hi, lo = split(value)
        ahi[at, pl.ds(0, rows), :] = hi
        alo[at, pl.ds(0, rows), :] = lo
        if spare:
            ahi[at, pl.ds(rows, spare), :] = hi[rows - spare :]
            alo[at, pl.ds(rows, spare), :] = lo[rows - spare :]

    def band(s):
        return turned[pl.ds(pl.multiple_of(s * rows, 8), rows), :depth]

    def turn(k):
        def step(j, _):
            base = pl.multiple_of(j * TURN, TURN)
            turned[pl.ds(base, TURN), :] = raw[k, :, pl.ds(base, TURN)].T
            return 0

        load(k).wait()
        if spare:
            load_spare(k).wait()
        lax.fori_loop(0, size // TURN, step, 0)

        def cut(s, _):
            store(k * n_row + s, band(s))
            return 0

        lax.fori_loop(0, n_row, cut, 0)

    def corners():
        column = lax.broadcasted_iota(jnp.int32, (rows, depth), 0)
        line = lax.broadcasted_iota(jnp.int32, (rows, depth), 1)
        line = line - jnp.where(line >= rows, spare, 0)
        value = band(r)
        store(c * n_row + r, jnp.where(column < line, value, jnp.where(column == line, 1.0, 0.0)))
        store(n_col * n_row, jnp.where(column >= line, value, 0.0))

    turn(c)
    corners()
    pl.semaphore_wait(barrier, n_row * n_col - 1)

    def enter(q):
        far_first(lambda row: to_row(rs_buf.at[q], v_buf, v_send, v_recv, q, row, c).start(), True, False, False)

    def each_of(g, body):
        def step(i, _):
            body(g * (chunks // GROUPS) + i)
            return 0

        lax.fori_loop(0, chunks // GROUPS, step, 0)

    @pl.when(c == 0)
    def _():
        each_of(0, enter)

    def first_run(q):
        return remote(rs_buf.at[q], rin.at[c, q], r_send.at[c, q], r_recv.at[c, q], r, 0)

    @pl.when(c > 0)
    def _():
        each_chunk(lambda q: first_run(q).start())

    def turn_others(i, _):
        turn(lax.rem(c + i, n_col))
        return 0

    lax.fori_loop(1, n_col, turn_others, 0)

    def back_run(q):
        return remote(f_buf.at[q, r], rbin.at[c, q], b0_send.at[q], rb_recv.at[c, q], r, last)

    def deliver(ref, q, value):
        ref[0, pl.ds(pl.multiple_of(q * portion, 8), portion), :] = value[:, :rows]

    def forward_of(own, is_last):
        def one(q):
            wait = functools.partial(arrivals, v_buf, v_recv, q, False, True, own)
            acc = combine_as_they_come(v_buf, tile(c), q, wait, 0)
            f_buf[q, r] = pack(acc)
            if is_last:
                far_first(lambda row: to_row(f_buf.at[q, r], f_buf, f_send, f_recv, q, row, c).start(), False, True, False)
            else:
                spread(lambda row: to_row(f_buf.at[q, r], f_buf, f_send, f_recv, q, row, c).start(), True)
                back_run(q).start()
            deliver(fwd_ref, q, acc)

        return one

    def wait_run(run, recv, k, q):
        remote(run.at[k, q], run.at[k, q], recv.at[k, q], recv.at[k, q], r, c).wait_recv()

    def sweep_of(buf, recv, count, step, run_in, run_recv, run_out, run_send, stage, out, send, out_recv):
        nxt = c + step

        def one(q):
            wait = functools.partial(gather, buf, recv, q, step > 0)
            acc = combine_as_they_come(buf, tile(nxt), q, wait, n_row - 1 if step > 0 else 0)
            wait_run(run_in, run_recv, nxt, q)
            stage[q] = run_in[nxt, q] - pack(acc)
            far_first(
                lambda row: to_row(stage.at[q], out, send, out_recv, q, row, nxt).start(),
                step > 0, step < 0, True,
            )

        def rest(g):
            each = chunks // GROUPS

            def other(i, _):
                k = nxt + step * i
                acc = combine(buf, tile(k), g * each, each)
                for part in range(each):
                    q = g * each + part
                    wait_run(run_in, run_recv, k, q)
                    run_out[k, q] = run_in[k, q] - pack(acc[part * portion : (part + 1) * portion])
                    remote(run_out.at[k, q], run_in.at[k, q], run_send.at[k, q], run_recv.at[k, q], r, nxt).start()
                return 0

            lax.fori_loop(1, count, other, 0)

        return one, rest

    def backward_of(buf, recv, own, is_first):
        def one(q):
            wait = functools.partial(arrivals, buf, recv, q, True, False, own)
            acc = combine_as_they_come(buf, upper, q, wait, n_row - 1)
            if not is_first:
                s_buf[q, r] = pack(acc)
                spread(lambda row: to_row(s_buf.at[q, r], s_buf, s_send, s_recv, q, row, c).start(), False)
            deliver(sol_ref, q, acc)

        return one

    def pipeline(final, *stages):
        def step(t, _):
            for first, body in stages:
                @pl.when((t >= first) & (t < first + DELAY * GROUPS) & ((t + DELAY - first % DELAY) % DELAY == 0))
                def _():
                    if body in (down_rest, back_rest):
                        body((t - first) // DELAY)
                    else:
                        each_of((t - first) // DELAY, body)

            return 0

        lax.fori_loop(0, final + DELAY * (GROUPS - 1) + 1, step, 0)

    down, down_rest = sweep_of(f_buf, f_recv, last - c, 1, rin, r_recv, rout, r_send, t_buf, v_buf, w_send, v_recv)
    back, back_rest = sweep_of(s_buf, s_recv, c, -1, rbin, rb_recv, rbout, rb_send, tb_buf, w_buf, v_send, w_recv)

    pass_down = pass_on_of(f_buf, f_recv, True)
    pass_back = pass_on_of(s_buf, s_recv, False)

    @pl.when(c == 0)
    def _():
        def enter_next(q):
            @pl.when(q + chunks // GROUPS < chunks)
            def _():
                enter(q + chunks // GROUPS)

        pipeline(
            4 * last + 1,
            (1, pass_down), (1, down), (0, forward_of(False, False)), (DELAY - 1, enter_next), (1, down_rest),
            (4 * last + 1, backward_of(w_buf, w_recv, True, True)),
        )

    @pl.when((c > 0) & (c < last))
    def _():
        turned_back = 4 * (last - c) + 1
        pipeline(
            turned_back + 1,
            (turned_back + 1, pass_back), (turned_back + 1, back), (turned_back, backward_of(w_buf, w_recv, True, False)),
            (1, pass_down), (1, down), (0, forward_of(True, False)),
            (1, down_rest), (turned_back + 1, back_rest),
        )

    @pl.when(c == last)
    def _():
        pipeline(
            2,
            (2, pass_back), (2, back), (1, backward_of(f_buf, f_recv, False, False)), (0, forward_of(True, True)),
            (2, back_rest),
        )

    def sent(src, send):
        remote(src, src, send, send, r, c).wait_send()

    def finish(q):
        @pl.when(c == 0)
        def _():
            far_first(lambda row: sent(rs_buf.at[q], v_send.at[q, row]), True, False, False)

        @pl.when(c > 0)
        def _():
            sent(rs_buf.at[q], r_send.at[c, q])
            far_first(lambda row: sent(tb_buf.at[q], v_send.at[q, row]), False, True, True)
            spread(lambda row: sent(s_buf.at[q, r], s_send.at[q, row]), False)
            relayed(lambda s, row, slot: sent(s_buf.at[q, s], g_send.at[q, s, slot]), False)

        @pl.when(c < last)
        def _():
            spread(lambda row: sent(f_buf.at[q, r], f_send.at[q, row]), True)
            relayed(lambda s, row, slot: sent(f_buf.at[q, s], g_send.at[q, s, slot]), True)
            sent(f_buf.at[q, r], b0_send.at[q])
            far_first(lambda row: sent(t_buf.at[q], w_send.at[q, row]), True, False, True)

        @pl.when(c == last)
        def _():
            far_first(lambda row: sent(f_buf.at[q, r], f_send.at[q, row]), False, True, False)

        def run(k, _):
            @pl.when(k > c + 1)
            def _():
                sent(rout.at[k, q], r_send.at[k, q])

            @pl.when(k < c - 1)
            def _():
                sent(rbout.at[k, q], rb_send.at[k, q])

            return 0

        lax.fori_loop(0, n_col, run, 0)

    each_chunk(finish)


def local(n_row, n_col, factors, right_side):
    tiles, rows, size = factors.shape
    width = right_side.shape[2]
    chunks = CHUNKS
    portion = width // chunks
    spare = 64 if rows % 128 == 64 and portion % 16 == 0 else 0
    padded = -(-rows // 128) * 128
    depth = rows + spare

    vmem = pl.BlockSpec(memory_space=pltpu.VMEM)
    anywhere = pl.BlockSpec(memory_space=pl.ANY)
    block = (portion * depth // 128 - spare * portion // 128, 128) if spare else (portion, rows)
    gathered = pltpu.VMEM((chunks, n_row, *block), jnp.float32)
    staged = pltpu.VMEM((chunks, *block), jnp.float32)
    runs = pltpu.VMEM((tiles, chunks, *block), jnp.float32)
    weights = pltpu.VMEM((tiles * n_row + 1, depth, depth), jnp.bfloat16)
    dma = pltpu.SemaphoreType.DMA
    shape = jax.ShapeDtypeStruct((1, width, rows), jnp.float32)
    forward, backward = pl.pallas_call(
        functools.partial(kernel, n_row, n_col, chunks, rows, size, width, spare),
        out_shape=(shape, shape),
        in_specs=[anywhere, vmem],
        out_specs=(vmem, vmem),
        scratch_shapes=[
            pltpu.VMEM((tiles, padded, size), jnp.float32), pltpu.VMEM((size, padded), jnp.float32),
            weights, weights, staged,
            gathered, gathered, gathered, gathered, staged, staged, runs, runs, runs, runs,
            dma((tiles, 2)),
            *([dma((chunks, n_row))] * 8),
            *([dma((tiles, chunks))] * 4),
            dma((chunks,)), dma((chunks, n_row, n_row // 2) if 2 < n_row <= 8 else (1, 1, 1)),
        ],
        compiler_params=pltpu.CompilerParams(collective_id=0, has_side_effects=True, vmem_limit_bytes=60 << 20),
    )(factors, right_side.transpose(0, 2, 1))

    def keep(forward_ref, backward_ref, forward_out, backward_out):
        forward_out[...] = forward_ref[...]
        backward_out[...] = backward_ref[...]

    forward, backward = pl.pallas_call(
        keep, out_shape=(shape, shape), in_specs=[vmem, vmem], out_specs=(vmem, vmem)
    )(forward, backward)
    return forward.transpose(0, 2, 1), backward.transpose(0, 2, 1)


def solution(mesh):
    return jax.shard_map(
        functools.partial(local, mesh.shape["row"], mesh.shape["col"]),
        mesh=mesh,
        in_specs=(P("groups", "row", "col"), P(("groups", "col"), "row", None)),
        out_specs=(P(("groups", "col"), "row", None), P(("groups", "col"), "row", None)),
        check_vma=False,
    )
```

```python
import functools

import jax
import jax.numpy as jnp
from jax import lax
from jax.experimental import pallas as pl
from jax.experimental.pallas import tpu as pltpu
from jax.sharding import PartitionSpec as P

MESH = pl.DeviceIdType.MESH
CHUNKS = 6
TURN = 256
GROUPS = 2
DELAY = 3


def kernel(
    n_row, n_col, chunks, rows, size, width, spare,
    factors_hbm, rs_ref,
    fwd_ref, sol_ref,
    raw, turned, ahi, alo, rs_buf, v_buf, f_buf, w_buf, s_buf, t_buf, tb_buf, rin, rout, rbin, rbout,
    a_sem, v_send, v_recv, f_send, f_recv, w_send, w_recv, s_send, s_recv,
    r_send, r_recv, rb_send, rb_recv, b0_send, g_send,
):
    r = lax.axis_index("row")
    c = lax.axis_index("col")
    last = n_col - 1
    portion = width // chunks
    short = n_row <= 4
    depth = rows + spare
    whole = rows // 128

    def load(k):
        return pltpu.make_async_copy(factors_hbm.at[k], raw.at[k, pl.ds(0, rows), :], a_sem.at[k, 0])

    def load_spare(k):
        src = factors_hbm.at[k, pl.ds(rows - spare, spare), :]
        return pltpu.make_async_copy(src, raw.at[k, pl.ds(rows, spare), :], a_sem.at[k, 1])

    def start_load(i, _):
        load(lax.rem(c + i, n_col)).start()
        if spare:
            load_spare(lax.rem(c + i, n_col)).start()
        return 0

    lax.fori_loop(0, n_col, start_load, 0)

    barrier = pltpu.get_barrier_semaphore()

    def greet(i, _):
        rr, cc = i // n_col, i % n_col

        @pl.when(i != r * n_col + c)
        def _():
            pl.semaphore_signal(barrier, inc=1, device_id={"row": rr, "col": cc}, device_id_type=MESH)

        return 0

    lax.fori_loop(0, n_row * n_col, greet, 0)

    def remote(src, dst, send, recv, row, col):
        return pltpu.make_async_remote_copy(
            src_ref=src, dst_ref=dst, send_sem=send, recv_sem=recv,
            device_id={"row": row, "col": col}, device_id_type=MESH,
        )

    def each_chunk(body):
        def step(q, _):
            body(q)
            return 0

        lax.fori_loop(0, chunks, step, 0)

    def each_row(body, first=0, stop=n_row):
        def step(s, _):
            body(s)
            return 0

        lax.fori_loop(first, stop, step, 0, unroll=short)

    def far_first(body, up, down, own, top=None, bottom=None):
        def step(i, _):
            d = n_row - 1 - i
            if down:
                @pl.when(r - d >= (0 if bottom is None else bottom))
                def _():
                    body(r - d)

            if up:
                @pl.when(r + d <= (n_row - 1 if top is None else top))
                def _():
                    body(r + d)

            return 0

        lax.fori_loop(0, n_row - 1, step, 0, unroll=short)
        if own:
            body(r)

    relays = g_send.shape[1] > 1
    half = n_row // 2
    mirror = n_row - 1 - half

    def spread(body, ahead):
        if not relays:
            far_first(body, True, True, False)
        elif ahead:
            @pl.when(r < half)
            def _():
                far_first(body, True, True, False, top=half)

            @pl.when(r >= half)
            def _():
                far_first(body, True, True, False)
        else:
            @pl.when(r > mirror)
            def _():
                far_first(body, True, True, False, bottom=mirror)

            @pl.when(r <= mirror)
            def _():
                far_first(body, True, True, False)

    def relayed(body, ahead):
        if not relays:
            return
        if ahead:
            @pl.when(r == half)
            def _():
                for s in range(half):
                    for row in range(half + 1, n_row):
                        body(s, row, row - half - 1)
        else:
            @pl.when(r == mirror)
            def _():
                for s in range(n_row - 1, mirror, -1):
                    for row in range(mirror):
                        body(s, row, row)

    def split(x):
        hi = x.astype(jnp.bfloat16)
        return hi, (x - hi.astype(jnp.float32)).astype(jnp.bfloat16)

    def halves(value):
        lane = lax.broadcasted_iota(jnp.int32, value.shape, 1)
        return lane < spare

    def unpack(block):
        if not spare:
            return block
        parts = [block[i * portion : (i + 1) * portion] for i in range(whole)]
        rest = block[whole * portion :]
        left = halves(rest)
        parts.append(jnp.concatenate([jnp.where(left, rest, 0.0), jnp.where(left, 0.0, rest)], axis=0))
        return jnp.concatenate(parts, axis=1)

    def pack(value):
        if not spare:
            return value
        parts = [value[:, i * 128 : (i + 1) * 128] for i in range(whole)]
        rest = value[:, whole * 128 :]
        top, low = rest[: portion // 2], rest[portion // 2 :]
        return jnp.concatenate([*parts, jnp.where(halves(top), top, low)], axis=0)

    def combine(buf, index, q, count=1, first=0, stop=n_row, start=None):
        portion = width // chunks * count

        def step(s, acc):
            hi, lo = split(jnp.concatenate([unpack(buf[q + i, s]) for i in range(count)], axis=0))
            both = jnp.concatenate([hi, lo], axis=0)
            one = jnp.dot(both, ahi[index(s)], preferred_element_type=jnp.float32)
            two = jnp.dot(hi, alo[index(s)], preferred_element_type=jnp.float32)
            return acc + (one[:portion] + one[portion:] + two)

        if start is None:
            start = jnp.zeros((portion, depth), jnp.float32)
        return lax.fori_loop(first, stop, step, start, unroll=short)

    def combine_as_they_come(buf, index, q, wait, last_row):
        others = (1, n_row) if last_row == 0 else (0, n_row - 1)
        final = (last_row, last_row + 1)
        wait(*others)
        acc = combine(buf, index, q, 1, *others)
        wait(*final)
        return combine(buf, index, q, 1, *final, acc)

    def tile(k):
        return lambda s: k * n_row + s

    def upper(s):
        same = 1 // (1 + (s - r) * (s - r))
        return c * n_row + s + same * ((n_col - c) * n_row - s)

    def arrive(buf, recv, q, s):
        remote(buf.at[q, s], buf.at[q, s], recv.at[q, s], recv.at[q, s], r, c).wait_recv()

    def arrivals(buf, recv, q, up, down, own, first, stop):
        def one(s):
            wanted = None if own else s != r
            if not up:
                wanted = s <= r if own else s < r
            if not down:
                wanted = s >= r if own else s > r
            if wanted is None:
                arrive(buf, recv, q, s)
            else:
                @pl.when(wanted)
                def _():
                    arrive(buf, recv, q, s)

        each_row(one, first, stop)

    def gather(buf, recv, q, ahead, first, stop):
        def one(i):
            s = i if ahead else first + stop - 1 - i
            wanted = s != r
            if relays and ahead:
                wanted = wanted & ((r != half) | (s > half))
            if relays and not ahead:
                wanted = wanted & ((r != mirror) | (s < mirror))

            @pl.when(wanted)
            def _():
                arrive(buf, recv, q, s)

        each_row(one, first, stop)

    def relay(buf, recv, q, s, row, slot):
        return remote(buf.at[q, s], buf.at[q, s], g_send.at[q, s, slot], recv.at[q, s], row, c)

    def pass_on_of(buf, recv, ahead):
        def one(q):
            def step(s, row, slot):
                if slot == 0:
                    arrive(buf, recv, q, s)
                relay(buf, recv, q, s, row, slot).start()

            relayed(step, ahead)

        return one

    def to_row(src, buf, send, recv, q, row, col):
        return remote(src, buf.at[q, r], send.at[q, row], recv.at[q, r], row, col)

    def prepare(q):
        value = rs_ref[0, pl.ds(pl.multiple_of(q * portion, 8), portion), :]
        if spare:
            value = jnp.concatenate([value, value[:, rows - spare :]], axis=1)
        rs_buf[q] = pack(value)

        @pl.when(c == 0)
        def _():
            v_buf[q, r] = rs_buf[q]

    each_chunk(prepare)

    def blank(s):
        zero = jnp.zeros((chunks, *v_buf.shape[2:]), jnp.float32)

        @pl.when(s > r)
        def _():
            v_buf[:, s] = zero

        @pl.when(s < r)
        def _():
            w_buf[:, s] = zero

            @pl.when(c == last)
            def _():
                f_buf[:, s] = zero

    each_row(blank)

    def store(at, value):
        hi, lo = split(value)
        ahi[at, pl.ds(0, rows), :] = hi
        alo[at, pl.ds(0, rows), :] = lo
        if spare:
            ahi[at, pl.ds(rows, spare), :] = hi[rows - spare :]
            alo[at, pl.ds(rows, spare), :] = lo[rows - spare :]

    def band(s):
        return turned[pl.ds(pl.multiple_of(s * rows, 8), rows), :depth]

    def turn(k):
        def step(j, _):
            base = pl.multiple_of(j * TURN, TURN)
            turned[pl.ds(base, TURN), :] = raw[k, :, pl.ds(base, TURN)].T
            return 0

        load(k).wait()
        if spare:
            load_spare(k).wait()
        lax.fori_loop(0, size // TURN, step, 0)

        def cut(s, _):
            store(k * n_row + s, band(s))
            return 0

        lax.fori_loop(0, n_row, cut, 0)

    def corners():
        column = lax.broadcasted_iota(jnp.int32, (rows, depth), 0)
        line = lax.broadcasted_iota(jnp.int32, (rows, depth), 1)
        line = line - jnp.where(line >= rows, spare, 0)
        value = band(r)
        store(c * n_row + r, jnp.where(column < line, value, jnp.where(column == line, 1.0, 0.0)))
        store(n_col * n_row, jnp.where(column >= line, value, 0.0))

    turn(c)
    corners()
    pl.semaphore_wait(barrier, n_row * n_col - 1)

    def enter(q):
        far_first(lambda row: to_row(rs_buf.at[q], v_buf, v_send, v_recv, q, row, c).start(), True, False, False)

    def each_of(g, body):
        def step(i, _):
            body(g * (chunks // GROUPS) + i)
            return 0

        lax.fori_loop(0, chunks // GROUPS, step, 0)

    @pl.when(c == 0)
    def _():
        each_of(0, enter)

    def first_run(q):
        return remote(rs_buf.at[q], rin.at[c, q], r_send.at[c, q], r_recv.at[c, q], r, 0)

    @pl.when(c > 0)
    def _():
        each_chunk(lambda q: first_run(q).start())

    def turn_others(i, _):
        turn(lax.rem(c + i, n_col))
        return 0

    lax.fori_loop(1, n_col, turn_others, 0)

    def back_run(q):
        return remote(f_buf.at[q, r], rbin.at[c, q], b0_send.at[q], rb_recv.at[c, q], r, last)

    def deliver(ref, q, value):
        ref[0, pl.ds(pl.multiple_of(q * portion, 8), portion), :] = value[:, :rows]

    def forward_of(own, is_last):
        def one(q):
            wait = functools.partial(arrivals, v_buf, v_recv, q, False, True, own)
            acc = combine_as_they_come(v_buf, tile(c), q, wait, 0)
            f_buf[q, r] = pack(acc)
            if is_last:
                far_first(lambda row: to_row(f_buf.at[q, r], f_buf, f_send, f_recv, q, row, c).start(), False, True, False)
            else:
                spread(lambda row: to_row(f_buf.at[q, r], f_buf, f_send, f_recv, q, row, c).start(), True)
                back_run(q).start()
            deliver(fwd_ref, q, acc)

        return one

    def wait_run(run, recv, k, q):
        remote(run.at[k, q], run.at[k, q], recv.at[k, q], recv.at[k, q], r, c).wait_recv()

    def sweep_of(buf, recv, count, step, run_in, run_recv, run_out, run_send, stage, out, send, out_recv):
        nxt = c + step

        def one(q):
            wait = functools.partial(gather, buf, recv, q, step > 0)
            acc = combine_as_they_come(buf, tile(nxt), q, wait, n_row - 1 if step > 0 else 0)
            wait_run(run_in, run_recv, nxt, q)
            stage[q] = run_in[nxt, q] - pack(acc)
            far_first(
                lambda row: to_row(stage.at[q], out, send, out_recv, q, row, nxt).start(),
                step > 0, step < 0, True,
            )

        def rest(g):
            each = chunks // GROUPS

            def other(i, _):
                k = nxt + step * i
                acc = combine(buf, tile(k), g * each, each)
                for part in range(each):
                    q = g * each + part
                    wait_run(run_in, run_recv, k, q)
                    run_out[k, q] = run_in[k, q] - pack(acc[part * portion : (part + 1) * portion])
                    remote(run_out.at[k, q], run_in.at[k, q], run_send.at[k, q], run_recv.at[k, q], r, nxt).start()
                return 0

            lax.fori_loop(1, count, other, 0)

        return one, rest

    def backward_of(buf, recv, own, is_first):
        def one(q):
            wait = functools.partial(arrivals, buf, recv, q, True, False, own)
            acc = combine_as_they_come(buf, upper, q, wait, n_row - 1)
            if not is_first:
                s_buf[q, r] = pack(acc)
                spread(lambda row: to_row(s_buf.at[q, r], s_buf, s_send, s_recv, q, row, c).start(), False)
            deliver(sol_ref, q, acc)

        return one

    def pipeline(final, *stages):
        def step(t, _):
            for first, body in stages:
                @pl.when((t >= first) & (t < first + DELAY * GROUPS) & ((t + DELAY - first % DELAY) % DELAY == 0))
                def _():
                    if body in (down_rest, back_rest):
                        body((t - first) // DELAY)
                    else:
                        each_of((t - first) // DELAY, body)

            return 0

        lax.fori_loop(0, final + DELAY * (GROUPS - 1) + 1, step, 0)

    down, down_rest = sweep_of(f_buf, f_recv, last - c, 1, rin, r_recv, rout, r_send, t_buf, v_buf, w_send, v_recv)
    back, back_rest = sweep_of(s_buf, s_recv, c, -1, rbin, rb_recv, rbout, rb_send, tb_buf, w_buf, v_send, w_recv)

    def sent(src, send):
        remote(src, src, send, send, r, c).wait_send()

    def finish(q):
        @pl.when(c == 0)
        def _():
            far_first(lambda row: sent(rs_buf.at[q], v_send.at[q, row]), True, False, False)

        @pl.when(c > 0)
        def _():
            sent(rs_buf.at[q], r_send.at[c, q])
            far_first(lambda row: sent(tb_buf.at[q], v_send.at[q, row]), False, True, True)
            spread(lambda row: sent(s_buf.at[q, r], s_send.at[q, row]), False)
            relayed(lambda s, row, slot: sent(s_buf.at[q, s], g_send.at[q, s, slot]), False)

        @pl.when(c < last)
        def _():
            spread(lambda row: sent(f_buf.at[q, r], f_send.at[q, row]), True)
            relayed(lambda s, row, slot: sent(f_buf.at[q, s], g_send.at[q, s, slot]), True)
            sent(f_buf.at[q, r], b0_send.at[q])
            far_first(lambda row: sent(t_buf.at[q], w_send.at[q, row]), True, False, True)

        @pl.when(c == last)
        def _():
            far_first(lambda row: sent(f_buf.at[q, r], f_send.at[q, row]), False, True, False)

        def run(k, _):
            @pl.when(k > c + 1)
            def _():
                sent(rout.at[k, q], r_send.at[k, q])

            @pl.when(k < c - 1)
            def _():
                sent(rbout.at[k, q], rb_send.at[k, q])

            return 0

        lax.fori_loop(0, n_col, run, 0)

    pass_down = pass_on_of(f_buf, f_recv, True)
    pass_back = pass_on_of(s_buf, s_recv, False)

    @pl.when(c == 0)
    def _():
        def enter_next(q):
            @pl.when(q + chunks // GROUPS < chunks)
            def _():
                enter(q + chunks // GROUPS)

        pipeline(
            4 * last + 1,
            (1, pass_down), (1, down), (0, forward_of(False, False)), (0, enter_next), (1, down_rest),
            (4 * last, finish), (4 * last + 1, backward_of(w_buf, w_recv, True, True)),
        )

    @pl.when((c > 0) & (c < last))
    def _():
        turned_back = 4 * (last - c) + 1
        pipeline(
            turned_back + 1,
            (turned_back + 1, pass_back), (turned_back + 1, back), (turned_back, backward_of(w_buf, w_recv, True, False)),
            (1, pass_down), (1, down), (0, forward_of(True, False)),
            (1, down_rest), (turned_back + 1, back_rest),
        )

    @pl.when(c == last)
    def _():
        pipeline(
            2,
            (2, pass_back), (2, back), (1, backward_of(f_buf, f_recv, False, False)), (0, forward_of(True, True)),
            (2, back_rest),
        )

    @pl.when(c > 0)
    def _():
        each_chunk(finish)


def local(n_row, n_col, factors, right_side):
    tiles, rows, size = factors.shape
    width = right_side.shape[2]
    chunks = CHUNKS
    portion = width // chunks
    spare = 64 if rows % 128 == 64 and portion % 16 == 0 else 0
    padded = -(-rows // 128) * 128
    depth = rows + spare

    vmem = pl.BlockSpec(memory_space=pltpu.VMEM)
    anywhere = pl.BlockSpec(memory_space=pl.ANY)
    block = (portion * depth // 128 - spare * portion // 128, 128) if spare else (portion, rows)
    gathered = pltpu.VMEM((chunks, n_row, *block), jnp.float32)
    staged = pltpu.VMEM((chunks, *block), jnp.float32)
    runs = pltpu.VMEM((tiles, chunks, *block), jnp.float32)
    weights = pltpu.VMEM((tiles * n_row + 1, depth, depth), jnp.bfloat16)
    dma = pltpu.SemaphoreType.DMA
    shape = jax.ShapeDtypeStruct((1, width, rows), jnp.float32)
    forward, backward = pl.pallas_call(
        functools.partial(kernel, n_row, n_col, chunks, rows, size, width, spare),
        out_shape=(shape, shape),
        in_specs=[anywhere, vmem],
        out_specs=(vmem, vmem),
        scratch_shapes=[
            pltpu.VMEM((tiles, padded, size), jnp.float32), pltpu.VMEM((size, padded), jnp.float32),
            weights, weights, staged,
            gathered, gathered, gathered, gathered, staged, staged, runs, runs, runs, runs,
            dma((tiles, 2)),
            *([dma((chunks, n_row))] * 8),
            *([dma((tiles, chunks))] * 4),
            dma((chunks,)), dma((chunks, n_row, n_row // 2) if 2 < n_row <= 8 else (1, 1, 1)),
        ],
        compiler_params=pltpu.CompilerParams(collective_id=0, has_side_effects=True, vmem_limit_bytes=60 << 20),
    )(factors, right_side.transpose(0, 2, 1))

    def keep(forward_ref, backward_ref, forward_out, backward_out):
        forward_out[...] = forward_ref[...]
        backward_out[...] = backward_ref[...]

    forward, backward = pl.pallas_call(
        keep, out_shape=(shape, shape), in_specs=[vmem, vmem], out_specs=(vmem, vmem)
    )(forward, backward)
    return forward.transpose(0, 2, 1), backward.transpose(0, 2, 1)


def solution(mesh):
    return jax.shard_map(
        functools.partial(local, mesh.shape["row"], mesh.shape["col"]),
        mesh=mesh,
        in_specs=(P("groups", "row", "col"), P(("groups", "col"), "row", None)),
        out_specs=(P(("groups", "col"), "row", None), P(("groups", "col"), "row", None)),
        check_vma=False,
    )
```
